32 devices in a mesh: row: 4 (over y, core), col: 8 (over z, x).
Axes of the slice: x: 2, y: 2, z: 4, core: 2. Of those that a mesh axis runs over, the one named last changes fastest.
Arguments:
- sources: bfloat16 [4, 8, 4, 256, 256], P('row', 'col'), may hold values from -6 to 6
- history: bfloat16 [4, 8, 8, 256, 256], P(None, 'col'), may hold values from -4 to 4
- inverse_diagonal: float32 [4, 8, 256], P('row', 'col'), may hold values from 0.3 to 0.6
- far_cores: bfloat16 [4, 8, 32, 4, 8, 8, 32], P('row', None, None, None, 'col'), may hold values from -0.09375 to 0.09375
- target_basis: bfloat16 [4, 8, 256, 32], P('row', 'col'), may hold values from -1 to 1
- source_basis: bfloat16 [4, 8, 256, 32], P(None, 'col'), may hold values from -0.375 to 0.375
- near_blocks: bfloat16 [4, 8, 3, 256, 8, 256], P('row', 'col'), may hold values from -0.078125 to 0.078125
- near_tile: int32 [4, 8, 3], P('row', 'col'), may hold values from 0 to 3
- near_count: int32 [4, 8], P('row', 'col'), may hold values from 1 to 3, as said below
Outputs:
- new_steps: bfloat16 [4, 8, 4, 256, 256], P('row', 'col')
- energies: float32 [4, 256], replicated
The draws below stay inside these ranges and needn't reach their ends.
Inputs may be any that keep to these rules, and one draw needn't show every extreme that they name: Only slots below near_count are used; in every draw some tile has all 3 slots live.
All inputs are finite; a program needn't handle non-finite values.
Results may differ from the reference program's by a relative error of at most 0.011.
Values may be sent and summed in bfloat16 or wider, within the bound.
A program may use at most 192 MiB of HBM per device.

```python
import math
import jax
import jax.numpy as jnp
from jax import lax

TILE = 256
RANK = 32
LAGS = 8
STEPS = 4
SLOTS = 3
FIELDS = 256
PANELS = 8192
N_ROW = 4
N_COL = 8


def draw_near_count(key, part):
    first_key, other_key = jax.random.split(jax.random.fold_in(key, 7))
    counts = jax.random.randint(first_key, (N_ROW * N_COL,), 1, SLOTS + 1)
    chosen = jax.random.randint(other_key, (), 0, N_ROW * N_COL)
    counts = counts.at[chosen].set(SLOTS)
    return counts.reshape(N_ROW, N_COL).astype(jnp.int32)


def with_ends(values, own_key, smallest, largest):
    longest = values.shape.index(max(values.shape))
    spots = []
    for shift in (0, 1):
        where = [jax.random.randint(jax.random.fold_in(own_key, axis), (), 0, length) for axis, length in enumerate(values.shape)]
        where[longest] = (where[longest] + shift) % values.shape[longest]
        spots.append(tuple(where))
    return values.at[spots[0]].set(smallest).at[spots[1]].set(largest)


def strengthened(array, key, source, target, parts, factor):
    def block_of(position):
        return (jnp.arange(array.shape[position]) // (array.shape[position] // parts)).reshape((-1,) + (1,) * (array.ndim - 1 - position))

    first = jax.random.permutation(key, parts)[block_of(target)]
    second = (block_of(target) + parts // 2) % parts
    return jnp.where((block_of(source) == first) | (block_of(source) == second), factor * array, array)


def level_of(rng, shape, shards, smallest, top_value):
    def one(dim, blocks):
        draws = jax.random.uniform(jax.random.fold_in(jax.random.fold_in(rng, 6), dim), (blocks,), jnp.float32, smallest / len(shards), top_value / len(shards))
        return jnp.repeat(jnp.exp(draws), shape[dim] // blocks).reshape((-1,) + (1,) * (len(shape) - dim - 1))

    loudness = one(*shards[0])
    for cut in shards[1:]:
        loudness = loudness * one(*cut)
    return loudness


def noise(key, shape, spread, reach, cuts=(), held_as=jnp.bfloat16):
    factor_of = level_of(key, shape, cuts, -0.22, 0.18) if cuts else 1.0
    drawn = jax.random.normal(key, shape, jnp.float32) * spread * factor_of
    return jnp.minimum(jnp.maximum(drawn, -reach), reach).astype(held_as)


def noise_with(stream_key, shape, scale, limit, pieces, heavy, kind=jnp.bfloat16):
    result = scale * jax.random.normal(stream_key, shape, jnp.float32)
    if pieces:
        result = result * level_of(stream_key, shape, pieces, -0.22, 0.18)
    return jnp.clip(strengthened(result, jax.random.fold_in(stream_key, 3), *heavy), -limit, limit).astype(kind)


def setup_inputs(seed: int = 0) -> dict:
    seeds = jax.random.split(jax.random.key(seed), 10)
    return {
        "sources": noise(seeds[0], (N_ROW, N_COL, STEPS, TILE, FIELDS), 1.0, 6.0, ((0, 4), (1, 8))),
        "history": noise(seeds[1], (N_ROW, N_COL, LAGS, TILE, FIELDS), 0.5, 4.0, ((1, 8),)),
        "inverse_diagonal": jnp.clip(jnp.exp(math.log(0.6) - 0.6931472 * jax.random.uniform(seeds[2], (N_ROW, N_COL, TILE), jnp.float32) ** level_of(seeds[2], (N_ROW, N_COL, TILE), ((0, 4), (1, 8)), -0.2, 0.2)), 0.3, 0.6),
        "far_cores": noise_with(seeds[3], (N_ROW, N_COL, RANK, N_ROW, N_COL, LAGS, RANK), (N_ROW * N_COL * LAGS * RANK) ** -0.5, 0.09375, ((0, 4), (4, 8)), (4, 1, 8, 2.0)),
        "target_basis": noise(seeds[4], (N_ROW, N_COL, TILE, RANK), RANK ** -0.5, 1.0, ((0, 4), (1, 8))),
        "source_basis": noise(seeds[5], (N_ROW, N_COL, TILE, RANK), TILE ** -0.5, 0.375, ((1, 8),)),
        "near_blocks": noise(seeds[6], (N_ROW, N_COL, SLOTS, TILE, LAGS, TILE), (SLOTS * LAGS * TILE) ** -0.5, 0.078125, ((0, 4), (1, 8))),
        "near_tile": with_ends(jax.random.randint(seeds[7], (N_ROW, N_COL, SLOTS), 0, N_ROW), jax.random.fold_in(seeds[7], 1), 0, N_ROW - 1).astype(jnp.int32),
        "near_count": draw_near_count(jax.random.fold_in(seeds[9], 71), 0),
    }


def project(source_basis, blocks):
    return jnp.einsum("ijta,ijktx->ijkax", source_basis.astype(jnp.float32), blocks.astype(jnp.float32)).astype(jnp.bfloat16)


def reference(sources, history, inverse_diagonal, far_cores, target_basis, source_basis, near_blocks, near_tile, near_count):
    row_count = history.shape[0]
    col_count = history.shape[1]
    past = history
    projected = project(source_basis, past)
    flat_blocks = near_blocks.reshape(row_count * col_count, SLOTS, TILE, LAGS * TILE)
    flat_tiles = near_tile.reshape(row_count * col_count, SLOTS)
    flat_counts = near_count.reshape(row_count * col_count)
    col_ids = (jnp.arange(row_count * col_count, dtype=jnp.int32) % col_count).astype(jnp.int32)
    outputs = []
    energy_rows = []
    for moment in range(STEPS):
        stacked = projected.reshape(row_count * col_count * LAGS * RANK, FIELDS)

        def row_cores(cores_row):
            matrix = cores_row.reshape(col_count * RANK, row_count * col_count * LAGS * RANK)
            summed = jnp.dot(matrix, stacked, preferred_element_type=jnp.float32)
            return summed.astype(jnp.bfloat16).reshape(col_count, RANK, FIELDS)

        core_now = lax.map(row_cores, far_cores)
        far = jnp.einsum("ijta,ijax->ijtx", target_basis.astype(jnp.float32), core_now.astype(jnp.float32))

        def near_tile_sum(inputs):
            blocks, tiles, count, col_id = inputs
            column = lax.dynamic_index_in_dim(past, col_id, 1, keepdims=False)
            total = jnp.zeros((TILE, FIELDS), jnp.float32)
            for slot in range(SLOTS):
                source = lax.dynamic_index_in_dim(column, tiles[slot], 0, keepdims=False).reshape(LAGS * TILE, FIELDS)
                term = jnp.dot(blocks[slot], source, preferred_element_type=jnp.float32)
                total = total + jnp.where(slot < count, term, jnp.zeros_like(term))
            return total

        near = lax.map(near_tile_sum, (flat_blocks, flat_tiles, flat_counts, col_ids)).reshape(row_count, col_count, TILE, FIELDS)
        fresh = (inverse_diagonal[:, :, :, None] * (sources[:, :, moment].astype(jnp.float32) - far - near)).astype(jnp.bfloat16)
        outputs.append(fresh)
        energy_rows.append(jnp.sum(jnp.square(fresh.astype(jnp.float32)), axis=(0, 1, 2)) / PANELS)
        past = jnp.concatenate([fresh[:, :, None], past[:, :, :-1]], axis=2)
        projected = jnp.concatenate([project(source_basis, fresh[:, :, None]), projected[:, :, :-1]], axis=2)
    return jnp.stack(outputs, axis=2), jnp.stack(energy_rows, axis=0)
```

```python
import functools

import jax
import jax.numpy as jnp
from jax import lax
from jax.experimental import pallas as pl
from jax.experimental.pallas import tpu as pltpu
from jax.sharding import PartitionSpec as P

MESH = pl.DeviceIdType.MESH
F32 = jnp.float32
BF16 = jnp.bfloat16


def march(
    rows,
    cols,
    panel_total,
    tiles_ref,
    count_ref,
    basis_hbm,
    history_hbm,
    cores_hbm,
    near_hbm,
    target_hbm,
    scaling_hbm,
    sources_hbm,
    steps_ref,
    energy_ref,
    basis,
    history,
    cores,
    near_blocks,
    target,
    scaling_row,
    sources,
    scaling,
    past_proj,
    fresh_tiles,
    fresh_proj,
    core_out,
    core_in,
    near_sum,
    partial_sum,
    energy_own,
    energy_rows,
    energy_mid,
    energy_cols,
    load_sems,
    tile_send,
    tile_recv,
    pass_send,
    pass_recv,
    proj_send,
    proj_recv,
    core_send,
    core_recv,
    erow_send,
    erow_recv,
    ecol_send,
    ecol_recv,
):
    step_count = sources.shape[0]
    lag_count, _, rank, fields = past_proj.shape
    tile = history.shape[2]
    slot_count = near_blocks.shape[0]
    width = rows * rank
    my_row = lax.axis_index("row")
    my_col = lax.axis_index("col")
    partner = my_row + 1 - 2 * lax.rem(my_row, 2)

    def row_peer(d):
        return lax.rem(my_row + d, rows)

    def col_peer(d):
        return lax.rem(my_col + d, cols)

    loads = [
        pltpu.make_async_copy(src, dst, load_sems.at[n])
        for n, (src, dst) in enumerate(
            (
                (basis_hbm, basis),
                (history_hbm, history),
                (cores_hbm, cores),
                (near_hbm, near_blocks),
                (target_hbm, target),
                (scaling_hbm, scaling_row),
                (sources_hbm, sources),
            )
        )
    ]
    for load in loads:
        load.start()

    barrier = pltpu.get_barrier_semaphore()
    for d in range(1, rows):
        pl.semaphore_signal(barrier, inc=1, device_id={"row": row_peer(d)}, device_id_type=MESH)
    for d in range(1, cols):
        pl.semaphore_signal(barrier, inc=1, device_id={"col": col_peer(d)}, device_id_type=MESH)

    def row_copy(src, dst, send, recv, to):
        return pltpu.make_async_remote_copy(
            src_ref=src, dst_ref=dst, send_sem=send, recv_sem=recv,
            device_id={"row": to}, device_id_type=MESH,
        )

    def col_copy(src, dst, send, recv, to):
        return pltpu.make_async_remote_copy(
            src_ref=src, dst_ref=dst, send_sem=send, recv_sem=recv,
            device_id={"col": to}, device_id_type=MESH,
        )

    def proj_copy(n, owner, d):
        return row_copy(
            fresh_proj.at[n, owner], fresh_proj.at[n, owner],
            proj_send.at[n, d], proj_recv.at[n, owner], row_peer(d),
        )

    def tile_copy(n, owner, d):
        return row_copy(
            fresh_tiles[n].at[owner], fresh_tiles[n].at[owner],
            tile_send.at[n, d], tile_recv.at[n, owner], row_peer(d),
        )

    def pass_copy(n, owner):
        return row_copy(
            fresh_tiles[n].at[owner], fresh_tiles[n].at[owner],
            pass_send.at[n, owner], pass_recv.at[n, owner], partner,
        )

    def core_copy(n, d):
        to = col_peer(d)
        return col_copy(
            core_out.at[n, to], core_in.at[n, my_col],
            core_send.at[n, d], core_recv.at[n, my_col], to,
        )

    def core_arrival(n, origin):
        return col_copy(
            core_out.at[n, origin], core_in.at[n, origin],
            core_send.at[n, 0], core_recv.at[n, origin], origin,
        )

    def far_base(n):
        depth = lag_count - n
        total = jnp.dot(
            cores[:, n * width:],
            past_proj[0:depth].reshape(depth * width, fields),
            preferred_element_type=F32,
        )
        for lag in range(1, n):
            total += jnp.dot(
                cores[:, lag * width:(lag + 1) * width],
                fresh_proj[n - 1 - lag].reshape(width, fields),
                preferred_element_type=F32,
            )
        return total

    def near_base(n):
        depth = lag_count - n

        def add_slot(slot, carry):
            where = tiles_ref[slot]
            value = jnp.dot(
                near_blocks[slot, :, n * tile:],
                history[where, 0:depth].reshape(depth * tile, fields),
                preferred_element_type=F32,
            )
            for lag in range(1, n):
                value += jnp.dot(
                    near_blocks[slot, :, lag * tile:(lag + 1) * tile],
                    fresh_tiles[n - 1 - lag][where],
                    preferred_element_type=F32,
                )
            near_sum[n] += jnp.where(slot < count_ref[0], value, 0.0)
            return carry

        near_sum[n] = jnp.zeros((tile, fields), F32)
        lax.fori_loop(0, slot_count, add_slot, 0)

    def near_fresh(n):
        def add_slot(slot, carry):
            value = jnp.dot(
                near_blocks[slot, :, 0:tile],
                fresh_tiles[n - 1][tiles_ref[slot]],
                preferred_element_type=F32,
            )
            near_sum[n] += jnp.where(slot < count_ref[0], value, 0.0)
            return carry

        lax.fori_loop(0, slot_count, add_slot, 0)

    loads[0].wait()
    loads[1].wait()

    def project_lag(lag, carry):
        for p in range(rows):
            past_proj[lag, p] = jnp.dot(
                basis[p], history[p, lag], preferred_element_type=F32
            ).astype(BF16)
        return carry

    lax.fori_loop(0, lag_count, project_lag, 0)
    loads[2].wait()

    for n in range(step_count):
        if n == 0:
            partial = far_base(0)
        else:
            for d in range(1, rows):
                proj_copy(n - 1, row_peer(d), d).wait_recv()
            partial = partial_sum[...] + jnp.dot(
                cores[:, 0:width],
                fresh_proj[n - 1].reshape(width, fields),
                preferred_element_type=F32,
            )
        core_out[n] = partial.astype(BF16).reshape(cols, rank, fields)
        if n == 0:
            pl.semaphore_wait(barrier, rows - 1 + cols - 1)
        for d in range(1, cols):
            core_copy(n, d).start()
        if n == 0:
            loads[3].wait()
            near_base(0)
            loads[4].wait()
            loads[5].wait()
            loads[6].wait()
            scaling[...] = jnp.transpose(jnp.broadcast_to(scaling_row[...], (fields, tile)))
        else:
            for d in range(2, rows, 2):
                tile_copy(n - 1, row_peer(d), d).wait_recv()
                pass_copy(n - 1, row_peer(d)).start()
            tile_copy(n - 1, partner, 1).wait_recv()
            for d in range(2, rows, 2):
                pass_copy(n - 1, lax.rem(partner + d, rows)).wait_recv()
            near_fresh(n)
        core = core_out[n, my_col].astype(F32)
        for d in range(1, cols):
            origin = col_peer(d)
            core_arrival(n, origin).wait_recv()
            core += core_in[n, origin].astype(F32)
        far = lax.dot_general(
            target[...], core.astype(BF16), (((0,), (0,)), ((), ())),
            preferred_element_type=F32,
        )
        fresh = (scaling[...] * (sources[n].astype(F32) - far - near_sum[n])).astype(BF16)
        if n + 1 < step_count:
            fresh_tiles[n][my_row] = fresh
            row_copy(
                fresh_tiles[n].at[my_row], fresh_tiles[n].at[my_row],
                tile_send.at[n, 0], tile_recv.at[n, my_row], partner,
            ).start()
            fresh_proj[n, my_row] = jnp.dot(
                basis[my_row], fresh, preferred_element_type=F32
            ).astype(BF16)
            for d in range(1, rows):
                proj_copy(n, my_row, d).start()
            for d in range(2, rows, 2):
                tile_copy(n, my_row, d).start()
        steps_ref[n] = fresh
        energy_own[n:n + 1, :] = (
            jnp.sum(jnp.square(fresh.astype(F32)), axis=0, keepdims=True) / panel_total
        )
        if n + 1 < step_count:
            partial_sum[...] = far_base(n + 1)
            near_base(n + 1)

    def erow_copy(origin, d):
        return row_copy(
            energy_own, energy_rows.at[origin], erow_send.at[d], erow_recv.at[origin], row_peer(d)
        )

    def ecol_copy(origin, d):
        return col_copy(
            energy_mid, energy_cols.at[origin], ecol_send.at[d], ecol_recv.at[origin], col_peer(d)
        )

    for d in range(1, rows):
        erow_copy(my_row, d).start()
    energy_rows[my_row] = energy_own[...]
    for d in range(1, rows):
        erow_copy(row_peer(d), d).wait_recv()
    total = energy_rows[0]
    for p in range(1, rows):
        total += energy_rows[p]
    energy_mid[...] = total
    for d in range(1, cols):
        ecol_copy(my_col, d).start()
    energy_cols[my_col] = total
    for d in range(1, cols):
        ecol_copy(col_peer(d), d).wait_recv()
    total = energy_cols[0]
    for q in range(1, cols):
        total += energy_cols[q]
    energy_ref[...] = total

    for n in range(step_count):
        for d in range(1, cols):
            core_copy(n, d).wait_send()
        if n + 1 < step_count:
            row_copy(
                fresh_tiles[n].at[my_row], fresh_tiles[n].at[my_row],
                tile_send.at[n, 0], tile_recv.at[n, my_row], partner,
            ).wait_send()
            for d in range(1, rows):
                proj_copy(n, my_row, d).wait_send()
            for d in range(2, rows, 2):
                tile_copy(n, my_row, d).wait_send()
                pass_copy(n, row_peer(d)).wait_send()
    for d in range(1, rows):
        erow_copy(my_row, d).wait_send()
    for d in range(1, cols):
        ecol_copy(my_col, d).wait_send()


def local(
    sources,
    history,
    inverse_diagonal,
    far_cores,
    target_basis,
    source_basis,
    near_blocks,
    near_tile,
    near_count,
):
    rows, _, lags, tile, fields = history.shape
    cols, rank = far_cores.shape[1:3]
    steps = sources.shape[2]
    slots = near_blocks.shape[2]
    panel_total = rows * cols * tile
    cores = jnp.transpose(far_cores.reshape(cols * rank, rows, lags, rank), (0, 2, 1, 3)).reshape(
        cols * rank, lags * rows * rank
    )
    near = near_blocks.reshape(slots, tile, lags * tile)
    dma = pltpu.SemaphoreType.DMA
    anywhere = pl.BlockSpec(memory_space=pl.ANY)
    scalar = pl.BlockSpec(memory_space=pltpu.SMEM)
    inside = pl.BlockSpec(memory_space=pltpu.VMEM)
    new_steps, energies = pl.pallas_call(
        functools.partial(march, rows, cols, panel_total),
        out_shape=(
            jax.ShapeDtypeStruct((steps, tile, fields), BF16),
            jax.ShapeDtypeStruct((steps, fields), F32),
        ),
        in_specs=[scalar, scalar] + [anywhere] * 7,
        out_specs=(inside, inside),
        scratch_shapes=[
            pltpu.VMEM((rows, rank, tile), BF16),
            pltpu.VMEM((rows, lags, tile, fields), BF16),
            pltpu.VMEM((cols * rank, lags * rows * rank), BF16),
            pltpu.VMEM((slots, tile, lags * tile), BF16),
            pltpu.VMEM((rank, tile), BF16),
            pltpu.VMEM((1, tile), F32),
            pltpu.VMEM((steps, tile, fields), BF16),
            pltpu.VMEM((tile, fields), F32),
            pltpu.VMEM((lags, rows, rank, fields), BF16),
            tuple(pltpu.VMEM((rows, tile, fields), BF16) for _ in range(steps - 1)),
            pltpu.VMEM((steps - 1, rows, rank, fields), BF16),
            pltpu.VMEM((steps, cols, rank, fields), BF16),
            pltpu.VMEM((steps, cols, rank, fields), BF16),
            pltpu.VMEM((steps, tile, fields), F32),
            pltpu.VMEM((cols * rank, fields), F32),
            pltpu.VMEM((steps, fields), F32),
            pltpu.VMEM((rows, steps, fields), F32),
            pltpu.VMEM((steps, fields), F32),
            pltpu.VMEM((cols, steps, fields), F32),
            dma((7,)),
            dma((steps - 1, rows)),
            dma((steps - 1, rows)),
            dma((steps - 1, rows)),
            dma((steps - 1, rows)),
            dma((steps - 1, rows)),
            dma((steps - 1, rows)),
            dma((steps, cols)),
            dma((steps, cols)),
            dma((rows,)),
            dma((rows,)),
            dma((cols,)),
            dma((cols,)),
        ],
        compiler_params=pltpu.CompilerParams(
            collective_id=0, has_side_effects=True, vmem_limit_bytes=56 * 1024 * 1024
        ),
    )(
        near_tile.reshape(slots),
        near_count.reshape(1),
        jnp.swapaxes(source_basis[:, 0], 1, 2),
        history[:, 0],
        cores,
        near,
        jnp.swapaxes(target_basis[0, 0], 0, 1),
        inverse_diagonal[0],
        sources[0, 0],
    )
    return new_steps[None, None], energies


def solution(mesh):
    placed = (
        P("row", "col", None, None, None),
        P(None, "col", None, None, None),
        P("row", "col", None),
        P("row", None, None, None, "col", None, None),
        P("row", "col", None, None),
        P(None, "col", None, None),
        P("row", "col", None, None, None, None),
        P("row", "col", None),
        P("row", "col"),
    )
    return jax.shard_map(
        local,
        mesh=mesh,
        in_specs=placed,
        out_specs=(P("row", "col", None, None, None), P()),
        check_vma=False,
    )
```

```python
import functools

import jax
import jax.numpy as jnp
from jax import lax
from jax.experimental import pallas as pl
from jax.experimental.pallas import tpu as pltpu
from jax.sharding import PartitionSpec as P

MESH = pl.DeviceIdType.MESH
F32 = jnp.float32
BF16 = jnp.bfloat16


def march(
    rows,
    cols,
    panel_total,
    tiles_ref,
    count_ref,
    basis_hbm,
    history_hbm,
    cores_hbm,
    near_hbm,
    target_hbm,
    scaling_hbm,
    sources_hbm,
    steps_ref,
    energy_ref,
    basis,
    history,
    cores,
    near_blocks,
    target,
    scaling_row,
    sources,
    scaling,
    cores_raw,
    near_raw,
    stage,
    past_proj,
    fresh_tiles,
    fresh_proj,
    core_out,
    core_in,
    near_sum,
    partial_sum,
    energy_own,
    energy_rows,
    energy_mid,
    energy_cols,
    load_sems,
    history_sems,
    tile_send,
    tile_recv,
    pass_send,
    pass_recv,
    proj_send,
    proj_recv,
    core_send,
    core_recv,
    erow_send,
    erow_recv,
    ecol_send,
    ecol_recv,
):
    step_count = sources.shape[0]
    lag_count, _, rank, fields = past_proj.shape
    tile = history.shape[2]
    slot_count = near_blocks.shape[0]
    width = rows * rank
    my_row = lax.axis_index("row")
    my_col = lax.axis_index("col")
    partner = my_row + 1 - 2 * lax.rem(my_row, 2)

    def row_peer(d):
        return lax.rem(my_row + d, rows)

    def col_peer(d):
        return lax.rem(my_col + d, cols)

    loads = [
        pltpu.make_async_copy(src, dst, load_sems.at[n])
        for n, (src, dst) in enumerate(
            (
                (basis_hbm, basis),
                (cores_hbm, cores_raw),
                (near_hbm, near_raw),
                (target_hbm, target),
                (scaling_hbm, scaling_row),
                (sources_hbm, sources),
            )
        )
    ]

    def history_load(lag):
        return pltpu.make_async_copy(
            history_hbm.at[:, lag], history.at[:, lag], history_sems.at[lag]
        )

    loads[0].start()
    loads[1].start()
    for lag in range(lag_count):
        history_load(lag).start()
    for load in loads[2:]:
        load.start()

    barrier = pltpu.get_barrier_semaphore()
    for d in range(1, rows):
        pl.semaphore_signal(barrier, inc=1, device_id={"row": row_peer(d)}, device_id_type=MESH)
    for d in range(1, cols):
        pl.semaphore_signal(barrier, inc=1, device_id={"col": col_peer(d)}, device_id_type=MESH)

    def row_copy(src, dst, send, recv, to):
        return pltpu.make_async_remote_copy(
            src_ref=src, dst_ref=dst, send_sem=send, recv_sem=recv,
            device_id={"row": to}, device_id_type=MESH,
        )

    def col_copy(src, dst, send, recv, to):
        return pltpu.make_async_remote_copy(
            src_ref=src, dst_ref=dst, send_sem=send, recv_sem=recv,
            device_id={"col": to}, device_id_type=MESH,
        )

    def proj_copy(n, owner, d):
        return row_copy(
            fresh_proj.at[n, owner], fresh_proj.at[n, owner],
            proj_send.at[n, d], proj_recv.at[n, owner], row_peer(d),
        )

    def tile_copy(n, owner, d):
        return row_copy(
            fresh_tiles[n].at[owner], fresh_tiles[n].at[owner],
            tile_send.at[n, d], tile_recv.at[n, owner], row_peer(d),
        )

    def pass_copy(n, owner):
        return row_copy(
            fresh_tiles[n].at[owner], fresh_tiles[n].at[owner],
            pass_send.at[n, owner], pass_recv.at[n, owner], partner,
        )

    def core_copy(n, d):
        to = col_peer(d)
        return col_copy(
            core_out.at[n, to], core_in.at[n, my_col],
            core_send.at[n, d], core_recv.at[n, my_col], to,
        )

    def core_arrival(n, origin):
        return col_copy(
            core_out.at[n, origin], core_in.at[n, origin],
            core_send.at[n, 0], core_recv.at[n, origin], origin,
        )

    def far_base(n):
        depth = lag_count - n
        total = jnp.dot(
            cores[:, n * width:],
            past_proj[0:depth].reshape(depth * width, fields),
            preferred_element_type=F32,
        )
        for lag in range(1, n):
            total += jnp.dot(
                cores[:, lag * width:(lag + 1) * width],
                fresh_proj[n - 1 - lag].reshape(width, fields),
                preferred_element_type=F32,
            )
        return total

    def near_base(n):
        depth = lag_count - n

        def add_slot(slot, carry):
            where = tiles_ref[slot]
            value = jnp.dot(
                near_blocks[slot, :, n * tile:],
                history[where, 0:depth].reshape(depth * tile, fields),
                preferred_element_type=F32,
            )
            for lag in range(1, n):
                value += jnp.dot(
                    near_blocks[slot, :, lag * tile:(lag + 1) * tile],
                    fresh_tiles[n - 1 - lag][where],
                    preferred_element_type=F32,
                )
            near_sum[n] += jnp.where(slot < count_ref[0], value, 0.0)
            return carry

        near_sum[n] = jnp.zeros((tile, fields), F32)
        lax.fori_loop(0, slot_count, add_slot, 0)

    def near_fresh(n):
        def add_slot(slot, carry):
            value = jnp.dot(
                near_blocks[slot, :, 0:tile],
                fresh_tiles[n - 1][tiles_ref[slot]],
                preferred_element_type=F32,
            )
            near_sum[n] += jnp.where(slot < count_ref[0], value, 0.0)
            return carry

        lax.fori_loop(0, slot_count, add_slot, 0)

    lanes = stage.shape[2]
    block = stage.shape[1] // lag_count

    def spread(value):
        for c in range(value.shape[1] // lanes):
            stage[c] = value[:, c * lanes:(c + 1) * lanes]

    def pick(lag, c):
        return stage[c, pl.ds(lag, block, stride=lag_count), :].astype(BF16)

    def pack_cores(g, carry):
        here = pl.ds(pl.multiple_of(g * block, block), block)
        total = None
        for p in range(rows):
            value = cores_raw[here, p].astype(F32).reshape(block * lag_count, rank).astype(BF16)
            place = (
                lax.broadcasted_iota(jnp.int32, (rank, width), 1)
                == lax.broadcasted_iota(jnp.int32, (rank, width), 0) + p * rank
            )
            term = jnp.dot(
                value, place.astype(F32).astype(BF16), preferred_element_type=F32
            )
            total = term if total is None else total + term
        spread(total)
        for lag in range(lag_count):
            for c in range(width // lanes):
                first = lag * width + c * lanes
                cores[here, first:first + lanes] = pick(lag, c)
        return carry

    def pack_near(index, carry):
        slot = index // (tile // block)
        here = pl.ds(pl.multiple_of(lax.rem(index, tile // block) * block, block), block)
        spread(near_raw[slot, here].astype(F32).reshape(block * lag_count, tile))
        for lag in range(lag_count):
            for c in range(tile // lanes):
                first = lag * tile + c * lanes
                near_blocks[slot, here, first:first + lanes] = pick(lag, c)
        return carry

    loads[1].wait()
    lax.fori_loop(0, cores.shape[0] // block, pack_cores, 0)
    loads[0].wait()

    def project_lag(lag, carry):
        history_load(lag).wait()
        for p in range(rows):
            past_proj[lag, p] = jnp.dot(
                basis[p], history[p, lag], preferred_element_type=F32
            ).astype(BF16)
        return carry

    lax.fori_loop(0, lag_count, project_lag, 0)

    for n in range(step_count):
        if n == 0:
            partial = far_base(0)
        else:
            for d in range(1, rows):
                proj_copy(n - 1, row_peer(d), d).wait_recv()
            partial = partial_sum[...] + jnp.dot(
                cores[:, 0:width],
                fresh_proj[n - 1].reshape(width, fields),
                preferred_element_type=F32,
            )
        core_out[n] = partial.astype(BF16).reshape(cols, rank, fields)
        if n == 0:
            pl.semaphore_wait(barrier, rows - 1 + cols - 1)
        for d in range(1, cols):
            core_copy(n, d).start()
        if n == 0:
            loads[2].wait()
            lax.fori_loop(0, slot_count * (tile // block), pack_near, 0)
            near_base(0)
            for load in loads[3:]:
                load.wait()
            scaling[...] = jnp.transpose(jnp.broadcast_to(scaling_row[...], (fields, tile)))
        else:
            near_base(n)
            for d in range(2, rows, 2):
                tile_copy(n - 1, row_peer(d), d).wait_recv()
                pass_copy(n - 1, row_peer(d)).start()
            tile_copy(n - 1, partner, 1).wait_recv()
            for d in range(2, rows, 2):
                pass_copy(n - 1, lax.rem(partner + d, rows)).wait_recv()
            near_fresh(n)
        core = core_out[n, my_col].astype(F32)
        for d in range(1, cols):
            origin = col_peer(d)
            core_arrival(n, origin).wait_recv()
            core += core_in[n, origin].astype(F32)
        far = lax.dot_general(
            target[...], core.astype(BF16), (((0,), (0,)), ((), ())),
            preferred_element_type=F32,
        )
        fresh = (scaling[...] * (sources[n].astype(F32) - far - near_sum[n])).astype(BF16)
        if n + 1 < step_count:
            fresh_tiles[n][my_row] = fresh
            row_copy(
                fresh_tiles[n].at[my_row], fresh_tiles[n].at[my_row],
                tile_send.at[n, 0], tile_recv.at[n, my_row], partner,
            ).start()
            fresh_proj[n, my_row] = jnp.dot(
                basis[my_row], fresh, preferred_element_type=F32
            ).astype(BF16)
            for d in range(1, rows):
                proj_copy(n, my_row, d).start()
            for d in range(2, rows, 2):
                tile_copy(n, my_row, d).start()
        steps_ref[n] = fresh
        energy_own[n:n + 1, :] = (
            jnp.sum(jnp.square(fresh.astype(F32)), axis=0, keepdims=True) / panel_total
        )
        if n + 1 < step_count:
            partial_sum[...] = far_base(n + 1)

    def erow_copy(origin, d):
        return row_copy(
            energy_own, energy_rows.at[origin], erow_send.at[d], erow_recv.at[origin], row_peer(d)
        )

    def ecol_copy(origin, d):
        return col_copy(
            energy_mid, energy_cols.at[origin], ecol_send.at[d], ecol_recv.at[origin], col_peer(d)
        )

    for d in range(1, rows):
        erow_copy(my_row, d).start()
    energy_rows[my_row] = energy_own[...]
    for d in range(1, rows):
        erow_copy(row_peer(d), d).wait_recv()
    total = energy_rows[0]
    for p in range(1, rows):
        total += energy_rows[p]
    energy_mid[...] = total
    for d in range(1, cols):
        ecol_copy(my_col, d).start()
    energy_cols[my_col] = total
    for d in range(1, cols):
        ecol_copy(col_peer(d), d).wait_recv()
    total = energy_cols[0]
    for q in range(1, cols):
        total += energy_cols[q]
    energy_ref[...] = total

    for n in range(step_count):
        for d in range(1, cols):
            core_copy(n, d).wait_send()
        if n + 1 < step_count:
            row_copy(
                fresh_tiles[n].at[my_row], fresh_tiles[n].at[my_row],
                tile_send.at[n, 0], tile_recv.at[n, my_row], partner,
            ).wait_send()
            for d in range(1, rows):
                proj_copy(n, my_row, d).wait_send()
            for d in range(2, rows, 2):
                tile_copy(n, my_row, d).wait_send()
                pass_copy(n, row_peer(d)).wait_send()
    for d in range(1, rows):
        erow_copy(my_row, d).wait_send()
    for d in range(1, cols):
        ecol_copy(my_col, d).wait_send()


def hand_over(steps_in, energy_in, steps_out, energy_out):
    steps_out[...] = steps_in[...]
    energy_out[...] = energy_in[...]


def local(
    sources,
    history,
    inverse_diagonal,
    far_cores,
    target_basis,
    source_basis,
    near_blocks,
    near_tile,
    near_count,
):
    rows, _, lags, tile, fields = history.shape
    cols, rank = far_cores.shape[1:3]
    steps = sources.shape[2]
    slots = near_blocks.shape[2]
    panel_total = rows * cols * tile
    lanes = min(128, tile, rows * rank)
    block = min(64, tile)
    dma = pltpu.SemaphoreType.DMA
    anywhere = pl.BlockSpec(memory_space=pltpu.HBM)
    scalar = pl.BlockSpec(memory_space=pltpu.SMEM)
    inside = pl.BlockSpec(memory_space=pltpu.VMEM)
    new_steps, energies = pl.pallas_call(
        functools.partial(march, rows, cols, panel_total),
        out_shape=(
            jax.ShapeDtypeStruct((steps, tile, fields), BF16),
            jax.ShapeDtypeStruct((steps, fields), F32),
        ),
        in_specs=[scalar, scalar] + [anywhere] * 7,
        out_specs=(inside, inside),
        scratch_shapes=[
            pltpu.VMEM((rows, rank, tile), BF16),
            pltpu.VMEM((rows, lags, tile, fields), BF16),
            pltpu.VMEM((cols * rank, lags * rows * rank), BF16),
            pltpu.VMEM((slots, tile, lags * tile), BF16),
            pltpu.VMEM((rank, tile), BF16),
            pltpu.VMEM((1, tile), F32),
            pltpu.VMEM((steps, tile, fields), BF16),
            pltpu.VMEM((tile, fields), F32),
            pltpu.VMEM((cols * rank, rows, lags, rank), BF16),
            pltpu.VMEM((slots, tile, lags, tile), BF16),
            pltpu.VMEM((max(tile, rows * rank) // lanes, block * lags, lanes), F32),
            pltpu.VMEM((lags, rows, rank, fields), BF16),
            tuple(pltpu.VMEM((rows, tile, fields), BF16) for _ in range(steps - 1)),
            pltpu.VMEM((steps - 1, rows, rank, fields), BF16),
            pltpu.VMEM((steps, cols, rank, fields), BF16),
            pltpu.VMEM((steps, cols, rank, fields), BF16),
            pltpu.VMEM((steps, tile, fields), F32),
            pltpu.VMEM((cols * rank, fields), F32),
            pltpu.VMEM((steps, fields), F32),
            pltpu.VMEM((rows, steps, fields), F32),
            pltpu.VMEM((steps, fields), F32),
            pltpu.VMEM((cols, steps, fields), F32),
            dma((6,)),
            dma((lags,)),
            dma((steps - 1, rows)),
            dma((steps - 1, rows)),
            dma((steps - 1, rows)),
            dma((steps - 1, rows)),
            dma((steps - 1, rows)),
            dma((steps - 1, rows)),
            dma((steps, cols)),
            dma((steps, cols)),
            dma((rows,)),
            dma((rows,)),
            dma((cols,)),
            dma((cols,)),
        ],
        compiler_params=pltpu.CompilerParams(
            collective_id=0, has_side_effects=True, vmem_limit_bytes=58 * 1024 * 1024
        ),
    )(
        near_tile.reshape(slots),
        near_count.reshape(1),
        jnp.swapaxes(source_basis[:, 0], 1, 2),
        history[:, 0],
        far_cores.reshape(cols * rank, rows, lags, rank),
        near_blocks[0, 0],
        jnp.swapaxes(target_basis[0, 0], 0, 1),
        inverse_diagonal[0],
        sources[0, 0],
    )
    new_steps, energies = pl.pallas_call(
        hand_over,
        out_shape=(
            jax.ShapeDtypeStruct((steps, tile, fields), BF16),
            jax.ShapeDtypeStruct((steps, fields), F32),
        ),
        in_specs=(inside, inside),
        out_specs=(inside, inside),
    )(new_steps, energies)
    return new_steps[None, None], energies


def solution(mesh):
    placed = (
        P("row", "col", None, None, None),
        P(None, "col", None, None, None),
        P("row", "col", None),
        P("row", None, None, None, "col", None, None),
        P("row", "col", None, None),
        P(None, "col", None, None),
        P("row", "col", None, None, None, None),
        P("row", "col", None),
        P("row", "col"),
    )
    return jax.shard_map(
        local,
        mesh=mesh,
        in_specs=placed,
        out_specs=(P("row", "col", None, None, None), P()),
        check_vma=False,
    )
```

```python
import functools

import jax
import jax.numpy as jnp
from jax import lax
from jax.experimental import pallas as pl
from jax.experimental.pallas import tpu as pltpu
from jax.sharding import PartitionSpec as P

MESH = pl.DeviceIdType.MESH
F32 = jnp.float32
BF16 = jnp.bfloat16


def march(
    rows,
    cols,
    panel_total,
    tiles_ref,
    count_ref,
    basis_hbm,
    history_hbm,
    cores_hbm,
    near_hbm,
    target_hbm,
    scaling_hbm,
    sources_hbm,
    steps_ref,
    energy_ref,
    basis,
    history,
    cores,
    near_blocks,
    target,
    scaling_row,
    sources,
    scaling,
    last_tile,
    cores_raw,
    near_raw,
    stage,
    past_proj,
    fresh_tiles,
    fresh_proj,
    core_out,
    core_in,
    near_sum,
    partial_sum,
    energy_own,
    energy_rows,
    energy_mid,
    energy_cols,
    load_sems,
    history_sems,
    result_sems,
    tile_send,
    tile_recv,
    pass_send,
    pass_recv,
    proj_send,
    proj_recv,
    core_send,
    core_recv,
    erow_send,
    erow_recv,
    ecol_send,
    ecol_recv,
):
    step_count = sources.shape[0]
    lag_count, _, rank, fields = past_proj.shape
    tile = history.shape[2]
    slot_count = near_blocks.shape[0]
    width = rows * rank
    my_row = lax.axis_index("row")
    my_col = lax.axis_index("col")
    partner = my_row + 1 - 2 * lax.rem(my_row, 2)

    def row_peer(d):
        return lax.rem(my_row + d, rows)

    def col_peer(d):
        return lax.rem(my_col + d, cols)

    loads = [
        pltpu.make_async_copy(src, dst, load_sems.at[n])
        for n, (src, dst) in enumerate(
            (
                (basis_hbm, basis),
                (cores_hbm, cores_raw),
                (near_hbm, near_raw),
                (target_hbm, target),
                (scaling_hbm, scaling_row),
                (sources_hbm, sources),
            )
        )
    ]

    def history_load(lag):
        return pltpu.make_async_copy(
            history_hbm.at[:, lag], history.at[:, lag], history_sems.at[lag]
        )

    loads[0].start()
    loads[1].start()
    for lag in range(lag_count):
        history_load(lag).start()
    for load in loads[2:]:
        load.start()

    barrier = pltpu.get_barrier_semaphore()
    for d in range(1, rows):
        pl.semaphore_signal(barrier, inc=1, device_id={"row": row_peer(d)}, device_id_type=MESH)
    for d in range(1, cols):
        pl.semaphore_signal(barrier, inc=1, device_id={"col": col_peer(d)}, device_id_type=MESH)

    def row_copy(src, dst, send, recv, to):
        return pltpu.make_async_remote_copy(
            src_ref=src, dst_ref=dst, send_sem=send, recv_sem=recv,
            device_id={"row": to}, device_id_type=MESH,
        )

    def col_copy(src, dst, send, recv, to):
        return pltpu.make_async_remote_copy(
            src_ref=src, dst_ref=dst, send_sem=send, recv_sem=recv,
            device_id={"col": to}, device_id_type=MESH,
        )

    def proj_copy(n, owner, d):
        return row_copy(
            fresh_proj.at[n, owner], fresh_proj.at[n, owner],
            proj_send.at[n, d], proj_recv.at[n, owner], row_peer(d),
        )

    def tile_copy(n, owner, d):
        return row_copy(
            fresh_tiles[n].at[owner], fresh_tiles[n].at[owner],
            tile_send.at[n, d], tile_recv.at[n, owner], row_peer(d),
        )

    def pass_copy(n, owner):
        return row_copy(
            fresh_tiles[n].at[owner], fresh_tiles[n].at[owner],
            pass_send.at[n, owner], pass_recv.at[n, owner], partner,
        )

    def core_copy(n, d):
        to = col_peer(d)
        return col_copy(
            core_out.at[n, to], core_in.at[n, my_col],
            core_send.at[n, d], core_recv.at[n, my_col], to,
        )

    def core_arrival(n, origin):
        return col_copy(
            core_out.at[n, origin], core_in.at[n, origin],
            core_send.at[n, 0], core_recv.at[n, origin], origin,
        )

    def result_copy(n):
        return pltpu.make_async_copy(
            fresh_tiles[n].at[my_row] if n + 1 < step_count else last_tile,
            steps_ref.at[n],
            result_sems.at[n],
        )

    def far_base(n):
        depth = lag_count - n
        total = jnp.dot(
            cores[:, n * width:],
            past_proj[0:depth].reshape(depth * width, fields),
            preferred_element_type=F32,
        )
        for lag in range(1, n):
            total += jnp.dot(
                cores[:, lag * width:(lag + 1) * width],
                fresh_proj[n - 1 - lag].reshape(width, fields),
                preferred_element_type=F32,
            )
        return total

    def near_base(n):
        depth = lag_count - n

        def add_slot(slot, carry):
            where = tiles_ref[slot]
            value = jnp.dot(
                near_blocks[slot, :, n * tile:],
                history[where, 0:depth].reshape(depth * tile, fields),
                preferred_element_type=F32,
            )
            for lag in range(1, n):
                value += jnp.dot(
                    near_blocks[slot, :, lag * tile:(lag + 1) * tile],
                    fresh_tiles[n - 1 - lag][where],
                    preferred_element_type=F32,
                )
            near_sum[n] += value
            return carry

        near_sum[n] = jnp.zeros((tile, fields), F32)
        lax.fori_loop(0, slot_count, add_slot, 0)

    def near_fresh(n):
        total = near_sum[n]
        for slot in range(slot_count):
            total += jnp.dot(
                near_blocks[slot, :, 0:tile],
                fresh_tiles[n - 1][tiles_ref[slot]],
                preferred_element_type=F32,
            )
        near_sum[n] = sources[n].astype(F32) - total

    lanes = stage.shape[2]
    block = stage.shape[1] // lag_count

    def spread(value):
        for c in range(value.shape[1] // lanes):
            stage[c] = value[:, c * lanes:(c + 1) * lanes]

    def pick(lag, c):
        return stage[c, pl.ds(lag, block, stride=lag_count), :].astype(BF16)

    def pack_cores(g, carry):
        here = pl.ds(pl.multiple_of(g * block, block), block)
        total = None
        for p in range(rows):
            value = cores_raw[here, p].astype(F32).reshape(block * lag_count, rank).astype(BF16)
            place = (
                lax.broadcasted_iota(jnp.int32, (rank, width), 1)
                == lax.broadcasted_iota(jnp.int32, (rank, width), 0) + p * rank
            )
            term = jnp.dot(
                value, place.astype(F32).astype(BF16), preferred_element_type=F32
            )
            total = term if total is None else total + term
        spread(total)
        for lag in range(lag_count):
            for c in range(width // lanes):
                first = lag * width + c * lanes
                cores[here, first:first + lanes] = pick(lag, c)
        return carry

    def pack_near(index, carry):
        slot = index // (tile // block)
        here = pl.ds(pl.multiple_of(lax.rem(index, tile // block) * block, block), block)
        spread(near_raw[slot, here].astype(F32).reshape(block * lag_count, tile))
        for lag in range(lag_count):
            for c in range(tile // lanes):
                first = lag * tile + c * lanes
                near_blocks[slot, here, first:first + lanes] = jnp.where(
                    slot < count_ref[0], pick(lag, c), jnp.zeros((block, lanes), BF16)
                )
        return carry

    loads[1].wait()
    lax.fori_loop(0, cores.shape[0] // block, pack_cores, 0)
    loads[0].wait()

    def project_lag(lag, carry):
        history_load(lag).wait()
        for p in range(rows):
            past_proj[lag, p] = jnp.dot(
                basis[p], history[p, lag], preferred_element_type=F32
            ).astype(BF16)
        return carry

    lax.fori_loop(0, lag_count, project_lag, 0)

    for n in range(step_count):
        if n == 0:
            partial = far_base(0)
        else:
            for d in range(1, rows):
                proj_copy(n - 1, row_peer(d), d).wait_recv()
            partial = partial_sum[...] + jnp.dot(
                cores[:, 0:width],
                fresh_proj[n - 1].reshape(width, fields),
                preferred_element_type=F32,
            )
        core_out[n] = partial.astype(BF16).reshape(cols, rank, fields)
        if n == 0:
            pl.semaphore_wait(barrier, rows - 1 + cols - 1)
        for d in range(1, cols):
            core_copy(n, d).start()
        if n == 0:
            loads[2].wait()
            lax.fori_loop(0, slot_count * (tile // block), pack_near, 0)
            near_base(0)
            for load in loads[3:]:
                load.wait()
            scaling[...] = jnp.transpose(jnp.broadcast_to(scaling_row[...], (fields, tile)))
            near_sum[0] = sources[0].astype(F32) - near_sum[0]
        else:
            near_base(n)
            for d in range(2, rows, 2):
                tile_copy(n - 1, row_peer(d), d).wait_recv()
                pass_copy(n - 1, row_peer(d)).start()
            tile_copy(n - 1, partner, 1).wait_recv()
            for d in range(2, rows, 2):
                pass_copy(n - 1, lax.rem(partner + d, rows)).wait_recv()
            near_fresh(n)
        core = core_out[n, my_col].astype(F32)
        for d in range(1, cols):
            origin = col_peer(d)
            core_arrival(n, origin).wait_recv()
            core += core_in[n, origin].astype(F32)
        far = lax.dot_general(
            target[...], core.astype(BF16), (((0,), (0,)), ((), ())),
            preferred_element_type=F32,
        )
        fresh = (scaling[...] * (near_sum[n] - far)).astype(BF16)
        if n + 1 < step_count:
            fresh_tiles[n][my_row] = fresh
            row_copy(
                fresh_tiles[n].at[my_row], fresh_tiles[n].at[my_row],
                tile_send.at[n, 0], tile_recv.at[n, my_row], partner,
            ).start()
            fresh_proj[n, my_row] = jnp.dot(
                basis[my_row], fresh, preferred_element_type=F32
            ).astype(BF16)
            for d in range(1, rows):
                proj_copy(n, my_row, d).start()
            for d in range(2, rows, 2):
                tile_copy(n, my_row, d).start()
        else:
            last_tile[...] = fresh
        result_copy(n).start()
        energy_own[n:n + 1, :] = (
            jnp.sum(jnp.square(fresh.astype(F32)), axis=0, keepdims=True) / panel_total
        )
        if n + 1 < step_count:
            partial_sum[...] = far_base(n + 1)

    def erow_copy(origin, d):
        return row_copy(
            energy_own, energy_rows.at[origin], erow_send.at[d], erow_recv.at[origin], row_peer(d)
        )

    def ecol_copy(origin, d):
        return col_copy(
            energy_mid, energy_cols.at[origin], ecol_send.at[d], ecol_recv.at[origin], col_peer(d)
        )

    for d in range(1, rows):
        erow_copy(my_row, d).start()
    energy_rows[my_row] = energy_own[...]
    for d in range(1, rows):
        erow_copy(row_peer(d), d).wait_recv()
    total = energy_rows[0]
    for p in range(1, rows):
        total += energy_rows[p]
    energy_mid[...] = total
    for d in range(1, cols):
        ecol_copy(my_col, d).start()
    energy_cols[my_col] = total
    for d in range(1, cols):
        ecol_copy(col_peer(d), d).wait_recv()
    total = energy_cols[0]
    for q in range(1, cols):
        total += energy_cols[q]
    energy_ref[...] = total

    for n in range(step_count):
        result_copy(n).wait()
        for d in range(1, cols):
            core_copy(n, d).wait_send()
        if n + 1 < step_count:
            row_copy(
                fresh_tiles[n].at[my_row], fresh_tiles[n].at[my_row],
                tile_send.at[n, 0], tile_recv.at[n, my_row], partner,
            ).wait_send()
            for d in range(1, rows):
                proj_copy(n, my_row, d).wait_send()
            for d in range(2, rows, 2):
                tile_copy(n, my_row, d).wait_send()
                pass_copy(n, row_peer(d)).wait_send()
    for d in range(1, rows):
        erow_copy(my_row, d).wait_send()
    for d in range(1, cols):
        ecol_copy(my_col, d).wait_send()


def hand_over(steps_in, energy_in, steps_out, energy_out):
    steps_out[...] = steps_in[...]
    energy_out[...] = energy_in[...]


def local(
    sources,
    history,
    inverse_diagonal,
    far_cores,
    target_basis,
    source_basis,
    near_blocks,
    near_tile,
    near_count,
):
    rows, _, lags, tile, fields = history.shape
    cols, rank = far_cores.shape[1:3]
    steps = sources.shape[2]
    slots = near_blocks.shape[2]
    panel_total = rows * cols * tile
    lanes = min(128, tile, rows * rank)
    block = min(64, tile)
    dma = pltpu.SemaphoreType.DMA
    anywhere = pl.BlockSpec(memory_space=pltpu.HBM)
    scalar = pl.BlockSpec(memory_space=pltpu.SMEM)
    inside = pl.BlockSpec(memory_space=pltpu.VMEM)
    new_steps, energies = pl.pallas_call(
        functools.partial(march, rows, cols, panel_total),
        out_shape=(
            jax.ShapeDtypeStruct((steps, tile, fields), BF16),
            jax.ShapeDtypeStruct((steps, fields), F32),
        ),
        in_specs=[scalar, scalar] + [anywhere] * 7,
        out_specs=(anywhere, inside),
        scratch_shapes=[
            pltpu.VMEM((rows, rank, tile), BF16),
            pltpu.VMEM((rows, lags, tile, fields), BF16),
            pltpu.VMEM((cols * rank, lags * rows * rank), BF16),
            pltpu.VMEM((slots, tile, lags * tile), BF16),
            pltpu.VMEM((rank, tile), BF16),
            pltpu.VMEM((1, tile), F32),
            pltpu.VMEM((steps, tile, fields), BF16),
            pltpu.VMEM((tile, fields), F32),
            pltpu.VMEM((tile, fields), BF16),
            pltpu.VMEM((cols * rank, rows, lags, rank), BF16),
            pltpu.VMEM((slots, tile, lags, tile), BF16),
            pltpu.VMEM((max(tile, rows * rank) // lanes, block * lags, lanes), F32),
            pltpu.VMEM((lags, rows, rank, fields), BF16),
            tuple(pltpu.VMEM((rows, tile, fields), BF16) for _ in range(steps - 1)),
            pltpu.VMEM((steps - 1, rows, rank, fields), BF16),
            pltpu.VMEM((steps, cols, rank, fields), BF16),
            pltpu.VMEM((steps, cols, rank, fields), BF16),
            pltpu.VMEM((steps, tile, fields), F32),
            pltpu.VMEM((cols * rank, fields), F32),
            pltpu.VMEM((steps, fields), F32),
            pltpu.VMEM((rows, steps, fields), F32),
            pltpu.VMEM((steps, fields), F32),
            pltpu.VMEM((cols, steps, fields), F32),
            dma((6,)),
            dma((lags,)),
            dma((steps,)),
            dma((steps - 1, rows)),
            dma((steps - 1, rows)),
            dma((steps - 1, rows)),
            dma((steps - 1, rows)),
            dma((steps - 1, rows)),
            dma((steps - 1, rows)),
            dma((steps, cols)),
            dma((steps, cols)),
            dma((rows,)),
            dma((rows,)),
            dma((cols,)),
            dma((cols,)),
        ],
        compiler_params=pltpu.CompilerParams(
            collective_id=0, has_side_effects=True, vmem_limit_bytes=58 * 1024 * 1024
        ),
    )(
        near_tile.reshape(slots),
        near_count.reshape(1),
        jnp.swapaxes(source_basis[:, 0], 1, 2),
        history[:, 0],
        far_cores.reshape(cols * rank, rows, lags, rank),
        near_blocks[0, 0],
        jnp.swapaxes(target_basis[0, 0], 0, 1),
        inverse_diagonal[0],
        sources[0, 0],
    )
    new_steps, energies = pl.pallas_call(
        hand_over,
        out_shape=(
            jax.ShapeDtypeStruct((steps, tile, fields), BF16),
            jax.ShapeDtypeStruct((steps, fields), F32),
        ),
        in_specs=(inside, inside),
        out_specs=(inside, inside),
    )(new_steps, energies)
    return new_steps[None, None], energies


def solution(mesh):
    placed = (
        P("row", "col", None, None, None),
        P(None, "col", None, None, None),
        P("row", "col", None),
        P("row", None, None, None, "col", None, None),
        P("row", "col", None, None),
        P(None, "col", None, None),
        P("row", "col", None, None, None, None),
        P("row", "col", None),
        P("row", "col"),
    )
    return jax.shard_map(
        local,
        mesh=mesh,
        in_specs=placed,
        out_specs=(P("row", "col", None, None, None), P()),
        check_vma=False,
    )
```
